256 devices in a mesh: ctx: 64 (over z, x, core), heads: 4 (over y).
Axes of the slice: x: 4, y: 4, z: 8, core: 2. Of those that a mesh axis runs over, the one named last changes fastest.
Arguments:
- query_rows: bfloat16 [64, 16, 2, 128], P('ctx', 'heads'), may hold values from -6 to 6
- past_keys: bfloat16 [64, 16, 4096, 128], P(None, 'heads', 'ctx'), may hold values from -6 to 6
- past_values: bfloat16 [64, 16, 4096, 128], P(None, 'heads', 'ctx'), may hold values from -6 to 6
- used_length: int32 [64], replicated, may hold values from 2048 to 4096
Outputs:
- read: bfloat16 [64, 16, 2, 128], P('ctx', 'heads')
The draws below stay inside these ranges and needn't reach their ends.
All inputs are finite; a program needn't handle non-finite values.
Results may differ from the reference program's by a relative error of at most 0.0015.
Values may be sent and summed in bfloat16 or wider, within the bound.
No kernel may reach another device: no remote copies, remote signals or barrier semaphores. Data moves between devices by JAX's collectives and lax.ppermute only.
A program may use at most 64 MiB of HBM per device.

```python
import jax
import jax.numpy as jnp
from jax import lax

BATCH = 64
LENGTH = 4096
KV_HEADS = 16
GROUP = 2
HEAD_SIZE = 128


def set_ends(result, key, least, largest):
    place = [jax.random.randint(jax.random.fold_in(key, axis), (), 0, length) for axis, length in enumerate(result.shape)]
    main_axis = result.shape.index(max(result.shape))
    beside = place[:main_axis] + [(place[main_axis] + 1) % result.shape[main_axis]] + place[main_axis + 1:]
    return result.at[tuple(place)].set(least).at[tuple(beside)].set(largest)


def shard_levels(stream_key, extent, pieces, least, largest):
    def one(position, shards_of):
        draws = jax.random.uniform(jax.random.fold_in(jax.random.fold_in(stream_key, 6), position), (shards_of,), jnp.float32, least / len(pieces), largest / len(pieces))
        return jnp.repeat(jnp.exp(draws), extent[position] // shards_of).reshape((-1,) + (1,) * (len(extent) - position - 1))

    factor_of = one(*pieces[0])
    for cut in pieces[1:]:
        factor_of = factor_of * one(*cut)
    return factor_of


def gaussian(rng, shape, width, most, cuts=(), kind=jnp.bfloat16):
    drawn = width * jax.random.normal(rng, shape, jnp.float32)
    if cuts:
        drawn = drawn * shard_levels(rng, shape, cuts, -0.22, 0.18)
    return jnp.clip(drawn, -most, most).astype(kind)


def setup_inputs(seed: int = 0) -> dict:
    key_of = jax.random.split(jax.random.key(seed), 5)
    query_rows = gaussian(key_of[0], (BATCH, KV_HEADS, GROUP, HEAD_SIZE), 1.0, 6.0, ((0, 64), (1, 4)))
    past_keys = gaussian(key_of[1], (BATCH, KV_HEADS, LENGTH, HEAD_SIZE), 1.0, 6.0, ((1, 4), (2, 64)))
    past_values = gaussian(key_of[2], (BATCH, KV_HEADS, LENGTH, HEAD_SIZE), 1.0, 6.0, ((1, 4), (2, 64)))
    used_length = set_ends(jax.random.randint(key_of[3], (BATCH,), LENGTH // 2, LENGTH + 1), jax.random.fold_in(key_of[3], 1), LENGTH // 2, LENGTH).astype(jnp.int32)
    return dict(query_rows=query_rows, past_keys=past_keys, past_values=past_values, used_length=used_length)


def reference(query_rows, past_keys, past_values, used_length):
    def one_sequence(item):
        query_one, keys_one, values_one, length_one = item
        logit = jnp.einsum("kgd,ktd->kgt", query_one.astype(jnp.float32), keys_one.astype(jnp.float32)) * HEAD_SIZE ** -0.5
        logit = jnp.where(jnp.arange(LENGTH) < length_one, logit, -1e30)
        share = jax.nn.softmax(logit, axis=-1)
        return jnp.einsum("kgt,ktd->kgd", share, values_one.astype(jnp.float32), precision=lax.Precision.HIGHEST)
    read = lax.map(one_sequence, (query_rows, past_keys, past_values, used_length)).astype(jnp.bfloat16)
    return read
```

```python
import jax
import jax.numpy as jnp
from jax import lax
from jax.experimental import pallas as pl
from jax.experimental.pallas import tpu as pltpu
from jax.sharding import PartitionSpec as P

CTX = "ctx"
SCALE = 128 ** -0.5
EMPTY = -30000.0
GROUP_OF = 8


def split3(x):
    first = lax.reduce_precision(x, 5, 10)
    second = lax.reduce_precision(x - first, 5, 10)
    third = (x - first) - second
    return tuple(piece.astype(jnp.float16) for piece in (first, second, third))


def attend_kernel(used_ref, query_ref, key_ref, value_ref, data_ref, stat_ref):
    sequences, rows, _ = query_ref.shape
    spots = key_ref.shape[1]
    length = spots // (rows // 2)
    first = lax.axis_index(CTX) * length
    row_head = lax.broadcasted_iota(jnp.int32, (rows, spots), 0) // 2
    lane = lax.broadcasted_iota(jnp.int32, (rows, spots), 1)
    position = jnp.where(row_head == lane // length, first + lane % length, 1 << 30)
    seq_lane = lax.broadcasted_iota(jnp.int32, (rows, 128), 1)

    def group(step, stats):
        total_log, scale_log = stats
        base = step * GROUP_OF
        logits = []
        for i in range(GROUP_OF):
            b = base + i
            s = lax.dot_general(
                query_ref[b], key_ref[b], (((1,), (1,)), ((), ())),
                preferred_element_type=jnp.float32,
            )
            logits.append(jnp.where(position < used_ref[b], s, -1e30))
        for i in range(GROUP_OF):
            b = base + i
            s = logits[i]
            top = jnp.maximum(jnp.max(s, axis=1, keepdims=True), -1e9)
            part = jnp.exp((s - top) * SCALE)
            weight = jnp.sum(part, axis=1, keepdims=True)
            high = part.astype(jnp.bfloat16)
            low = (part - high.astype(jnp.float32)).astype(jnp.bfloat16)
            both = lax.dot_general(
                jnp.concatenate([high, low], axis=0), value_ref[b], (((1,), (0,)), ((), ())),
                preferred_element_type=jnp.float32,
            )
            read = both[:rows] + both[rows:]
            most = jnp.max(jnp.abs(read), axis=1, keepdims=True)
            some = most > 0.0
            data_ref[b] = (read * jnp.where(some, 1.0 / jnp.where(some, most, 1.0), 0.0)).astype(data_ref.dtype)
            level = top * SCALE
            log_weight = jnp.where(weight > 0.0, level + jnp.log(weight), EMPTY)
            log_scale = jnp.where(some, level + jnp.log(most), EMPTY)
            here = seq_lane == b
            total_log = jnp.where(here, log_weight, total_log)
            scale_log = jnp.where(here, log_scale, scale_log)
        return total_log, scale_log

    zero = jnp.zeros((rows, 128), jnp.float32)
    total_log, scale_log = lax.fori_loop(0, sequences // GROUP_OF, group, (zero, zero))
    stat_ref[0] = total_log
    stat_ref[1] = scale_log


def attend(used_length, queries, keys, values):
    sequences, rows, width = queries.shape
    return pl.pallas_call(
        attend_kernel,
        out_shape=(
            jax.ShapeDtypeStruct((sequences, rows, width), jnp.float32),
            jax.ShapeDtypeStruct((2, rows, 128), jnp.float32),
        ),
        in_specs=[
            pl.BlockSpec(memory_space=pltpu.SMEM),
            pl.BlockSpec(memory_space=pltpu.VMEM),
            pl.BlockSpec(memory_space=pltpu.VMEM),
            pl.BlockSpec(memory_space=pltpu.VMEM),
        ],
        out_specs=(pl.BlockSpec(memory_space=pltpu.VMEM), pl.BlockSpec(memory_space=pltpu.VMEM)),
        cost_estimate=pl.CostEstimate(flops=10**9, bytes_accessed=9 * 2**20, transcendentals=10**5),
        name="attend",
    )(used_length, queries, keys, values)


def body(query_rows, past_keys, past_values, used_length):
    _, heads, group, width = query_rows.shape
    sequences, _, length, _ = past_keys.shape
    rows = heads * group
    own = jnp.broadcast_to(query_rows.reshape(1, rows, width), (sequences, rows, width))
    queries = lax.all_to_all(own, CTX, split_axis=0, concat_axis=0, tiled=True)
    data, stats = attend(
        used_length, queries,
        past_keys.reshape(sequences, heads * length, width),
        past_values.reshape(sequences, heads * length, width),
    )
    logs = stats[:, :, :sequences].transpose(2, 0, 1).reshape(sequences, 2 * rows)
    pieces = jnp.concatenate(split3(logs), axis=1)
    pieces = jnp.pad(pieces, ((0, 0), (0, group * width - pieces.shape[1]))).reshape(sequences, 1, group, width)
    message = jnp.concatenate([data.astype(jnp.float16).reshape(sequences, heads, group, width), pieces], axis=1)
    got = lax.all_to_all(message, CTX, split_axis=0, concat_axis=0, tiled=True)
    data = got[:, :heads].astype(jnp.float32).reshape(sequences, rows, width)
    logs = got[:, heads].astype(jnp.float32).reshape(sequences, group * width)[:, : 6 * rows]
    logs = logs.reshape(sequences, 3, 2, rows)
    logs = logs[:, 0] + logs[:, 1] + logs[:, 2]
    best = jnp.max(logs[:, 0], axis=0)
    weight = jnp.sum(jnp.exp(logs[:, 0] - best), axis=0)
    read = jnp.sum(data * jnp.exp(logs[:, 1] - best)[..., None], axis=0)
    return (read / weight[:, None]).astype(jnp.bfloat16).reshape(1, heads, group, width)


def solution(mesh):
    return jax.shard_map(
        body,
        mesh=mesh,
        in_specs=(
            P(CTX, "heads", None, None),
            P(None, "heads", CTX, None),
            P(None, "heads", CTX, None),
            P(),
        ),
        out_specs=P(CTX, "heads", None, None),
        check_vma=False,
    )
```

```python
import jax
import jax.numpy as jnp
from jax import lax
from jax.experimental import pallas as pl
from jax.experimental.pallas import tpu as pltpu
from jax.sharding import PartitionSpec as P

CTX = "ctx"
SCALE = 128 ** -0.5
EMPTY = -30000.0
CHUNK = 16


def split3(x):
    first = jnp.round(x * 2.0) * 0.5
    second = jnp.round((x - first) * 4096.0) * (1.0 / 4096.0)
    return first, second, (x - first) - second


def attend_kernel(
    used_hbm, query_ref, key_hbm, value_hbm, data_ref,
    used_ref, key_ref, value_ref, logit_ref, used_sem, key_sem, value_sem,
):
    sequences, rows, _ = query_ref.shape
    spots = key_ref.shape[1]
    length = spots // (rows // 2)
    chunks = sequences // CHUNK

    def load(source, target, sems, c):
        span = pl.ds(c * CHUNK, CHUNK)
        return pltpu.make_async_copy(source.at[span], target.at[span], sems.at[c])

    lengths = pltpu.make_async_copy(used_hbm, used_ref, used_sem)
    lengths.start()
    for c in range(chunks + 1):
        if c < chunks:
            load(key_hbm, key_ref, key_sem, c).start()
        if c > 0:
            load(value_hbm, value_ref, value_sem, c - 1).start()

    first = lax.axis_index(CTX) * length
    row_head = lax.broadcasted_iota(jnp.int32, (rows, spots), 0) // 2
    lane = lax.broadcasted_iota(jnp.int32, (rows, spots), 1)
    position = jnp.where(row_head == lane // length, first + lane % length, 1 << 30)
    seq_lane = lax.broadcasted_iota(jnp.int32, (rows, 128), 1)

    def score(b):
        s = lax.dot_general(
            query_ref[b], key_ref[b], (((1,), (1,)), ((), ())), preferred_element_type=jnp.float32
        )
        logit_ref[b] = jnp.where(position < used_ref[b], s, -1e30)

    def read(b, total_log, scale_log):
        s = logit_ref[b]
        top = jnp.maximum(jnp.max(s, axis=1, keepdims=True), -1e9)
        part = jnp.exp((s - top) * SCALE)
        weight = jnp.sum(part, axis=1, keepdims=True)
        high = part.astype(jnp.bfloat16)
        low = (part - high.astype(jnp.float32)).astype(jnp.bfloat16)
        both = lax.dot_general(
            jnp.concatenate([high, low], axis=0), value_ref[b], (((1,), (0,)), ((), ())),
            preferred_element_type=jnp.float32,
        )
        total = both[:rows] + both[rows:]
        most = jnp.max(jnp.abs(total), axis=1, keepdims=True)
        some = most > 0.0
        data_ref[b, : rows // 2] = (total * jnp.where(some, 1.0 / jnp.where(some, most, 1.0), 0.0)).reshape(rows // 2, 2, 128)
        level = top * SCALE
        here = seq_lane == b
        total_log = jnp.where(here, jnp.where(weight > 0.0, level + jnp.log(weight), EMPTY), total_log)
        scale_log = jnp.where(here, jnp.where(some, level + jnp.log(most), EMPTY), scale_log)
        return total_log, scale_log

    total_log = scale_log = jnp.zeros((rows, 128), jnp.float32)
    lengths.wait()
    for c in range(chunks + 1):
        if c < chunks:
            load(key_hbm, key_ref, key_sem, c).wait()
        if c > 0:
            load(value_hbm, value_ref, value_sem, c - 1).wait()
        for i in range(CHUNK):
            if c < chunks:
                score(c * CHUNK + i)
            if c > 0:
                total_log, scale_log = read((c - 1) * CHUNK + i, total_log, scale_log)
    pieces = [piece for pair in zip(split3(total_log), split3(scale_log)) for piece in pair]
    pieces += [jnp.zeros((128 - 6 * rows, 128), jnp.float32)]
    stats = jnp.concatenate(pieces, axis=0).T[:sequences]
    data_ref[:, rows // 2] = jnp.broadcast_to(stats[:, None, :], (sequences, 2, 128))


def in_hbm(x):
    return pltpu.with_memory_space_constraint(x, pltpu.HBM)


def attend(used_length, queries, keys, values):
    sequences, rows, width = queries.shape
    vmem = pl.BlockSpec(memory_space=pltpu.VMEM)
    chunks = sequences // CHUNK
    return pl.pallas_call(
        attend_kernel,
        out_shape=jax.ShapeDtypeStruct((sequences, rows // 2 + 1, 2, width), jnp.float32),
        in_specs=[
            pl.BlockSpec(memory_space=pltpu.HBM),
            vmem,
            pl.BlockSpec(memory_space=pltpu.HBM),
            pl.BlockSpec(memory_space=pltpu.HBM),
        ],
        out_specs=vmem,
        scratch_shapes=[
            pltpu.SMEM(used_length.shape, used_length.dtype),
            pltpu.VMEM(keys.shape, keys.dtype),
            pltpu.VMEM(values.shape, values.dtype),
            pltpu.VMEM((sequences, rows, keys.shape[1]), jnp.float32),
            pltpu.SemaphoreType.DMA,
            pltpu.SemaphoreType.DMA((chunks,)),
            pltpu.SemaphoreType.DMA((chunks,)),
        ],
        compiler_params=pltpu.CompilerParams(vmem_limit_bytes=16 * 2**20),
        cost_estimate=pl.CostEstimate(flops=10**9, bytes_accessed=9 * 2**20, transcendentals=10**5),
        name="attend",
    )(in_hbm(used_length), queries, in_hbm(keys), in_hbm(values))


def merge_kernel(got_ref, read_ref):
    sources, rows, _, _ = got_ref.shape
    rows = (rows - 1) * 2
    x = got_ref[:, rows // 2, 0]
    logs = x + pltpu.roll(x, 128 - 2 * rows, 1) + pltpu.roll(x, 128 - 4 * rows, 1)
    lane = lax.broadcasted_iota(jnp.int32, (1, 128), 1)
    best = jnp.max(logs, axis=0, keepdims=True)
    best = jnp.where(lane < rows, best, pltpu.roll(best, rows, 1))
    share = jnp.exp(jnp.where(lane < 2 * rows, logs - best, 0.0))
    total = pltpu.roll(jnp.sum(share, axis=0, keepdims=True), rows, 1)
    factor = jnp.concatenate([share / total, jnp.zeros((128 - sources, 128), jnp.float32)], axis=0).T
    factor = factor[rows : 2 * rows]
    sums = [jnp.zeros((rows, 128), jnp.float32) for _ in range(4)]
    for s in range(sources):
        sums[s % 4] += got_ref[s, : rows // 2].reshape(rows, 128) * factor[:, s : s + 1]
    read_ref[...] = ((sums[0] + sums[1]) + (sums[2] + sums[3])).astype(read_ref.dtype)


def merge(got):
    vmem = pl.BlockSpec(memory_space=pltpu.VMEM)
    return pl.pallas_call(
        merge_kernel,
        out_shape=jax.ShapeDtypeStruct((2 * got.shape[1] - 2, 128), jnp.bfloat16),
        in_specs=[vmem],
        out_specs=vmem,
        compiler_params=pltpu.CompilerParams(vmem_limit_bytes=4 * 2**20),
        name="merge",
    )(got)


def body(query_rows, past_keys, past_values, used_length):
    _, heads, group, width = query_rows.shape
    sequences, _, length, _ = past_keys.shape
    rows = heads * group
    own = jnp.broadcast_to(query_rows.reshape(1, rows, width), (sequences, rows, width))
    queries = lax.all_to_all(own, CTX, split_axis=0, concat_axis=0, tiled=True)
    message = attend(
        used_length, queries,
        past_keys.reshape(sequences, heads * length, width),
        past_values.reshape(sequences, heads * length, width),
    )
    got = lax.all_to_all(message.astype(jnp.float16), CTX, split_axis=0, concat_axis=0, tiled=True).astype(jnp.float32)
    read = merge(got)
    return read.reshape(1, heads, group, width)


def solution(mesh):
    return jax.shard_map(
        body,
        mesh=mesh,
        in_specs=(
            P(CTX, "heads", None, None),
            P(None, "heads", CTX, None),
            P(None, "heads", CTX, None),
            P(),
        ),
        out_specs=P(CTX, "heads", None, None),
        check_vma=False,
    )
```
